32 devices in a mesh: grp: 4 (over y, core), ep: 8 (over z, x).
Axes of the slice: x: 2, y: 2, z: 4, core: 2. Of those that a mesh axis runs over, the one named last changes fastest.
Arguments:
- d_out: bfloat16 [4096, 2048], P(('grp', 'ep')), may hold values from -12 to 12
- routes: int32 [4096, 2], P(('grp', 'ep')), may hold values from 0 to 7, all different within a row; in each aligned block of 128 rows (0 to 127, 128 to 255, ...) at most 48 rows name the same one
- combine: float32 [4096, 2], P(('grp', 'ep')), may hold values from 0.05 to 1
- live_tokens: int32 [32], P(('grp', 'ep')), may hold values from 1 to 128, as said below
- hidden: bfloat16 [1536, 57344], P('grp', 'ep'), may hold values from -6 to 6
Outputs:
- expert_grad: float32 [2048, 57344], P('grp', 'ep')
The draws below stay inside these ranges and needn't reach their ends.
Inputs may be any that keep to these rules, and one draw needn't show every extreme that they name: `routes`: the two experts of a token differ. Among the 128 rows of one device no expert is named by more than 48 rows, and on some devices one expert is named by exactly 48 rows. `live_tokens`: the live tokens of a device are its first ones; on the last device all 128 are live.
All inputs are finite; a program needn't handle non-finite values.
Results may differ from the reference program's by a relative error of at most 0.0029.
Values may be sent and summed in bfloat16 or wider, within the bound.
A program may use at most 128 MiB of HBM per device.

```python
import math
import jax
import jax.numpy as jnp
import numpy as np
from jax import lax

EXPERTS = 8
DW = 2048
H = 7168
TOK_DEV = 128
CAP = 48
SLOTS_E = 384
BLOCKS = 32
TOKENS = 4096
N_GRP = 4
N_EP = 8


def draw_live_tokens(key, part):
    index = jnp.arange(BLOCKS, dtype=jnp.int32)
    lowest = TOK_DEV // 4
    base = lowest + (TOK_DEV - lowest) * index // max(BLOCKS - 1, 1)
    jitter = jax.random.randint(jax.random.fold_in(key, 17), (BLOCKS,), 0, TOK_DEV // 8 + 1, dtype=jnp.int32)
    jitter = jnp.where(index == BLOCKS - 1, 0, jitter)
    return jnp.clip(base - jitter, 1, TOK_DEV).astype(jnp.int32)


def block_levels(key, extent, shards, low, top_value):
    def one(dim, blocks):
        draws = jax.random.uniform(jax.random.fold_in(jax.random.fold_in(key, 6), dim), (blocks,), jnp.float32, low / len(shards), top_value / len(shards))
        return jnp.repeat(jnp.exp(draws), extent[dim] // blocks).reshape((-1,) + (1,) * (len(extent) - dim - 1))

    factor_of = one(*shards[0])
    for cut in shards[1:]:
        factor_of = factor_of * one(*cut)
    return factor_of


def assign_block(key, own, number, rows, amount, top, most, skew):
    sequence = jax.random.permutation(key, amount)
    crowded, common = load_shares(amount, rows * top, most, skew, True), load_shares(amount, rows * top, most, skew, False)
    places = jnp.arange(amount)

    def named(sizes, offset_by):
        used = int((sizes > 0).sum())
        fixed = max(1, used // 4)
        moved = fixed + (places - fixed + offset_by * (used - fixed)) % max(1, amount - fixed)
        return jnp.zeros((amount,), jnp.int32).at[sequence[jnp.where(places < fixed, places, moved)]].set(jnp.asarray(sizes, jnp.int32))

    sizes = jnp.where(number % 4 == 0, named(crowded, number // 4), named(common, number - number // 4 - 1))
    mixed = jax.random.permutation(jax.random.fold_in(own, 3), amount)
    donor, taker = mixed[0:amount // 2 * 2:2], mixed[1:amount // 2 * 2:2]
    slack = jnp.minimum(sizes[donor] - 1, most - sizes[taker]) // 2
    slack = jnp.where((donor == sequence[0]) | (taker == sequence[0]) | (sizes[taker] == 0), 0, jnp.maximum(slack, 0))
    moved = jax.random.randint(jax.random.fold_in(own, 4), (amount // 2,), 0, 1 << 20) % (slack + 1)
    sizes = sizes.at[donor].add(-moved).at[taker].add(moved)
    items = jnp.searchsorted(jnp.cumsum(sizes), jnp.arange(rows * top), side="right").astype(jnp.int32)
    table = items.reshape(top, rows).T
    table = table[jax.random.permutation(jax.random.fold_in(own, 1), rows)]
    offset_by = jax.random.randint(jax.random.fold_in(own, 2), (rows, 1), 0, top)
    return jnp.take_along_axis(table, (jnp.arange(top)[None, :] + offset_by) % top, axis=1)


def load_shares(amount, total, bound, skew, full):
    portions = [(1 << 20) // math.isqrt(grade ** skew) + 1 for grade in range(1, amount + 1)]
    largest = bound if full else min(bound, max(-(-total // amount), total * portions[0] // sum(portions)))
    least = 1 if total - largest >= amount - 1 else 0
    given, spare = [largest] + [least] * (amount - 1), total - largest - least * (amount - 1)
    while spare > 0:
        movable = [i for i in range(1, amount) if given[i] < largest] or [i for i in range(1, amount) if given[i] < bound]
        whole, budget = sum([portions[i] for i in movable]), spare
        for i in movable:
            addition = min(bound - given[i], max(1, budget * portions[i] // whole), spare)
            given[i] = given[i] + addition
            spare = spare - addition
    return np.array(given)


def noise(own_key, extent, deviation, limit, shards=(), held_as=jnp.bfloat16):
    gain = block_levels(own_key, extent, shards, -0.22, 0.18) if shards else 1.0
    array = jax.random.normal(own_key, extent, jnp.float32) * deviation * gain
    return jnp.minimum(jnp.maximum(array, -limit), limit).astype(held_as)


def setup_inputs(seed: int = 0) -> dict:
    streams_of = jax.random.split(jax.random.key(seed), 6)
    d_out = noise(streams_of[0], (TOKENS, DW), 2.0, 12.0, ((0, 32),))
    routes_keys = jax.random.split(jax.random.fold_in(streams_of[1], 1), TOKENS // TOK_DEV)
    routes_turns = jax.random.permutation(jax.random.fold_in(streams_of[1], 3), TOKENS // TOK_DEV)
    routes = jax.vmap(lambda own, number: assign_block(jax.random.fold_in(streams_of[1], 2), own, number, TOK_DEV, EXPERTS, 2, CAP, 2))(routes_keys, routes_turns).reshape((TOKENS, 2))
    combine = jnp.clip(jnp.exp(math.log(1.0) - 2.9957323 * jax.random.uniform(streams_of[2], (TOKENS, 2), jnp.float32) ** block_levels(streams_of[2], (TOKENS, 2), ((0, 32),), -0.2, 0.2)), 0.05, 1.0)
    live_tokens = draw_live_tokens(jax.random.fold_in(streams_of[5], 71), 0)
    hidden = noise(streams_of[4], (N_GRP * SLOTS_E, EXPERTS * H), 1.0, 6.0, ((0, 4), (1, 8)))
    return dict(d_out=d_out, routes=routes, combine=combine, live_tokens=live_tokens, hidden=hidden)


def device_slots(d_rows, route_rows, weight_rows, live_count):
    tokens_here = d_rows.shape[0]
    alive = (jnp.arange(tokens_here, dtype=jnp.int32) < live_count).astype(jnp.float32)
    scaled = weight_rows * alive[:, None]
    weighted = (d_rows.astype(jnp.float32)[:, None, :] * scaled[:, :, None]).astype(jnp.bfloat16)
    weighted = weighted.reshape(tokens_here * route_rows.shape[1], d_rows.shape[1])
    flat = route_rows.reshape(-1).astype(jnp.int32)
    chosen = (flat[:, None] == jnp.arange(EXPERTS, dtype=jnp.int32)[None, :]).astype(jnp.int32)
    before = (jnp.cumsum(chosen, axis=0, dtype=jnp.int32) - chosen).astype(jnp.int32)
    position = lax.optimization_barrier(jnp.sum(before * chosen, axis=1, dtype=jnp.int32))
    slot_index = (flat * CAP + position).astype(jnp.int32)
    placing = (jnp.arange(EXPERTS * CAP, dtype=jnp.int32)[:, None] == slot_index[None, :]).astype(jnp.bfloat16)
    buffer = jnp.dot(placing, weighted, preferred_element_type=jnp.float32).astype(jnp.bfloat16)
    alive_pairs = jnp.repeat(alive, route_rows.shape[1])
    counts = lax.optimization_barrier(jnp.sum(chosen.astype(jnp.float32) * alive_pairs[:, None], axis=0))
    return (buffer.reshape(EXPERTS, CAP, d_rows.shape[1]), counts)

def reference(d_out, routes, combine, live_tokens, hidden):
    width = d_out.shape[1]
    group_tokens = N_EP * TOK_DEV

    def group_part(group):
        start = (group * group_tokens).astype(jnp.int32)
        rows = lax.dynamic_slice_in_dim(d_out, start, group_tokens, 0).reshape(N_EP, TOK_DEV, width)
        picks = lax.dynamic_slice_in_dim(routes, start, group_tokens, 0).reshape(N_EP, TOK_DEV, 2)
        weights = lax.dynamic_slice_in_dim(combine, start, group_tokens, 0).reshape(N_EP, TOK_DEV, 2)
        lives = lax.dynamic_slice_in_dim(live_tokens, (group * N_EP).astype(jnp.int32), N_EP, 0)
        buffers, counts = jax.vmap(device_slots)(rows, picks, weights, lives)

        def one_expert(expert):
            slots = lax.dynamic_index_in_dim(buffers, expert, 1, keepdims=False).reshape(N_EP * CAP, width)
            block = lax.dynamic_slice(hidden, ((group * SLOTS_E).astype(jnp.int32), (expert * H).astype(jnp.int32)), (SLOTS_E, H))
            return lax.dot_general(slots, block, (((0,), (0,)), ((), ())), preferred_element_type=jnp.float32)
        partial_value = lax.map(one_expert, jnp.arange(EXPERTS, dtype=jnp.int32))
        return (partial_value, lax.optimization_barrier(jnp.sum(counts, axis=0)))

    def step(carry, group):
        total, count = carry
        partial_value, counts = group_part(group)
        return ((total + partial_value, count + counts), None)
    start = (jnp.zeros((EXPERTS, width, H), jnp.float32), jnp.zeros((EXPERTS,), jnp.float32))
    (total, count), _ = lax.scan(step, start, jnp.arange(N_GRP, dtype=jnp.int32))
    result = total * lax.rsqrt(1.0 + count)[:, None, None]
    return jnp.transpose(result, (1, 0, 2)).reshape(width, EXPERTS * H)
```

```python
import functools

import jax
import jax.numpy as jnp
from jax import lax
from jax.experimental import pallas as pl
from jax.experimental.pallas import tpu as pltpu
from jax.sharding import PartitionSpec as P

EXPERTS = 8
CAP = 48
CORES = 2
CHUNKS = 7
MESH = pl.DeviceIdType.MESH


def pick_chunks(columns):
    return CHUNKS if columns % (CHUNKS * 128) == 0 else 1


def counts_kernel(n_grp, n_ep, mine, table, send_sem, recv_sem, own_sem):
    grp, ep = lax.axis_index("grp"), lax.axis_index("ep")
    total = n_grp * n_ep
    me = grp * n_ep + ep
    barrier = pltpu.get_barrier_semaphore()

    def place(j):
        other = lax.rem(me + j, total)
        return {"grp": other // n_ep, "ep": lax.rem(other, n_ep)}

    def greet(j, _):
        pl.semaphore_signal(barrier, inc=1, device_id=place(j), device_id_type=MESH)
        return 0

    lax.fori_loop(1, total, greet, 0)
    pl.semaphore_wait(barrier, total - 1)
    own = pltpu.make_async_copy(mine, table.at[me], own_sem)
    own.start()

    def copy(j):
        return pltpu.make_async_remote_copy(
            src_ref=mine, dst_ref=table.at[me], send_sem=send_sem.at[j], recv_sem=recv_sem.at[j],
            device_id=place(j), device_id_type=MESH)

    def send(j, _):
        copy(j).start()
        return 0

    def finish(j, _):
        copy(j).wait_send()
        source = lax.rem(me - j + total, total)
        pltpu.make_async_remote_copy(
            src_ref=mine, dst_ref=table.at[source], send_sem=send_sem.at[j], recv_sem=recv_sem.at[j],
            device_id=place(j), device_id_type=MESH).wait_recv()
        return 0

    lax.fori_loop(1, total, send, 0)
    lax.fori_loop(1, total, finish, 0)
    own.wait()


def share_counts(mine, n_grp, n_ep):
    total = n_grp * n_ep
    return pl.pallas_call(
        functools.partial(counts_kernel, n_grp, n_ep),
        out_shape=jax.ShapeDtypeStruct((total,) + mine.shape, mine.dtype),
        in_specs=[pl.BlockSpec(memory_space=pltpu.VMEM)],
        out_specs=pl.BlockSpec(memory_space=pltpu.VMEM),
        scratch_shapes=[
            pltpu.SemaphoreType.DMA((total,)),
            pltpu.SemaphoreType.DMA((total,)),
            pltpu.SemaphoreType.DMA,
        ],
        compiler_params=pltpu.CompilerParams(collective_id=0, has_side_effects=True),
        name="share_counts",
    )(mine)


def exchange_kernel(n_grp, n_ep, keep, sel, buffer, hidden, all_hidden, all_rows, arrived, packed, packed_rows,
                    slot_send, slot_recv, slot_own, far_send, far_recv, near_send, near_recv,
                    relay_send, relay_recv, row_send, row_recv, own_sem):
    n_y = n_grp // CORES
    grp, ep = lax.axis_index("grp"), lax.axis_index("ep")
    shards = n_ep // EXPERTS
    y = grp // CORES
    core = lax.rem(grp, CORES)
    pair = keep[0] + keep[1]
    chunks = pick_chunks(hidden.shape[1])
    wide = hidden.shape[1] // chunks
    block = all_rows.shape[1]

    barrier = pltpu.get_barrier_semaphore()

    def greet_ep(j, _):
        pl.semaphore_signal(barrier, inc=1, device_id={"grp": grp, "ep": lax.rem(ep + j, n_ep)}, device_id_type=MESH)
        return 0

    def greet_grp(j, _):
        pl.semaphore_signal(barrier, inc=1, device_id={"grp": lax.rem(grp + j, n_grp), "ep": ep}, device_id_type=MESH)
        return 0

    lax.fori_loop(1, n_ep, greet_ep, 0)
    lax.fori_loop(1, n_grp, greet_grp, 0)
    pl.semaphore_wait(barrier, n_ep - 1 + n_grp - 1)

    def slot_copy(j, source):
        target = lax.rem(ep + j, n_ep)
        return pltpu.make_async_remote_copy(
            src_ref=buffer.at[target // shards],
            dst_ref=arrived.at[pl.ds(pl.multiple_of(source * CAP, CAP), CAP), :],
            send_sem=slot_send.at[j], recv_sem=slot_recv.at[j],
            device_id={"grp": grp, "ep": target}, device_id_type=MESH)

    def slot_start(j, _):
        slot_copy(j, ep).start()
        return 0

    def slot_finish(j, _):
        slot_copy(j, ep).wait_send()
        slot_copy(j, lax.rem(ep - j + n_ep, n_ep)).wait_recv()
        return 0

    lax.fori_loop(1, n_ep, slot_start, 0)
    slot_mine = pltpu.make_async_copy(
        buffer.at[ep // shards], arrived.at[pl.ds(pl.multiple_of(ep * CAP, CAP), CAP), :], slot_own)
    slot_mine.start()

    def path(which):
        mine, other = keep[which], keep[1 - which]
        mate = y * CORES + (1 - which)

        def span(row, cell):
            start = row * pair + (0 if cell == 0 else keep[0])
            return pl.ds(pl.multiple_of(start, 16), keep[cell])

        def columns(i):
            return pl.ds(pl.multiple_of(i * wide, 128), wide)

        def at_y(j):
            return {"grp": lax.rem(y + j, n_y) * CORES + which, "ep": ep}

        def own_copy(i):
            return pltpu.make_async_copy(
                packed.at[pl.ds(0, mine), columns(i)], all_hidden.at[span(y, which), columns(i)], own_sem.at[i])

        def far_copy(j, i, row):
            return pltpu.make_async_remote_copy(
                src_ref=packed.at[pl.ds(0, mine), columns(i)], dst_ref=all_hidden.at[span(row, which), columns(i)],
                send_sem=far_send.at[j, i], recv_sem=far_recv.at[j, i], device_id=at_y(j), device_id_type=MESH)

        def near_copy(i):
            return pltpu.make_async_remote_copy(
                src_ref=packed.at[pl.ds(0, mine), columns(i)], dst_ref=all_hidden.at[span(y, which), columns(i)],
                send_sem=near_send.at[i], recv_sem=near_recv.at[i],
                device_id={"grp": mate, "ep": ep}, device_id_type=MESH)

        def near_arrival(i):
            return pltpu.make_async_remote_copy(
                src_ref=all_hidden.at[span(y, 1 - which), columns(i)],
                dst_ref=all_hidden.at[span(y, 1 - which), columns(i)],
                send_sem=near_send.at[i], recv_sem=near_recv.at[i],
                device_id={"grp": mate, "ep": ep}, device_id_type=MESH)

        def relay_copy(j, i, cell):
            row = lax.rem(y - j + n_y, n_y)
            return pltpu.make_async_remote_copy(
                src_ref=all_hidden.at[span(row, cell), columns(i)], dst_ref=all_hidden.at[span(row, cell), columns(i)],
                send_sem=relay_send.at[j, i], recv_sem=relay_recv.at[j, i],
                device_id={"grp": mate, "ep": ep}, device_id_type=MESH)

        def row_copy(j, k):
            cell = which if k == 0 else 1 - which
            target = lax.rem(y + j, n_y) * CORES + cell
            return pltpu.make_async_remote_copy(
                src_ref=packed_rows.at[pl.ds(0, mine), pl.ds(pl.multiple_of(target * block, 128), block)],
                dst_ref=all_rows.at[span(y, which), :],
                send_sem=row_send.at[j, k], recv_sem=row_recv.at[j, k],
                device_id={"grp": target, "ep": ep}, device_id_type=MESH)

        def row_arrival(j, k):
            cell = which if k == 0 else 1 - which
            here = all_rows.at[span(lax.rem(y - j + n_y, n_y), cell), :]
            return pltpu.make_async_remote_copy(
                src_ref=here, dst_ref=here, send_sem=row_send.at[j, k], recv_sem=row_recv.at[j, k],
                device_id={"grp": lax.rem(grp + 1, n_grp), "ep": ep}, device_id_type=MESH)

        others = [(j, k) for j in range(n_y) for k in range(CORES) if (j, k) != (0, 0)]

        def start(i):
            for j in range(1, n_y):
                far_copy(j, i, y).start()
            near_copy(i).start()
            own_copy(i).start()

        def pack(i, _):
            packed[pl.ds(0, mine), columns(i)] = jnp.dot(
                sel[pl.ds(0, mine), :], hidden[:, columns(i)], preferred_element_type=jnp.float32).astype(packed.dtype)

            @pl.when(i > 0)
            def _():
                start(i - 1)

            return 0

        lax.fori_loop(0, chunks, pack, 0)
        lax.fori_loop(1, n_ep, slot_finish, 0)
        slot_mine.wait()
        start(chunks - 1)

        def pack_rows(i, _):
            part = pl.ds(pl.multiple_of(i * block, 128), block)
            packed_rows[pl.ds(0, mine), part] = jnp.dot(
                sel[pl.ds(0, mine), :], arrived[:, part], preferred_element_type=jnp.float32).astype(packed_rows.dtype)
            return 0

        lax.fori_loop(0, n_grp, pack_rows, 0)
        row_mine = pltpu.make_async_copy(
            packed_rows.at[pl.ds(0, mine), pl.ds(pl.multiple_of(grp * block, 128), block)],
            all_rows.at[span(y, which), :], own_sem.at[chunks])
        for j, k in others:
            row_copy(j, k).start()
        row_mine.start()

        def relay(i, _):
            for j in range(1, n_y):
                far_copy(j, i, lax.rem(y - j + n_y, n_y)).wait_recv()
                relay_copy(j, i, which).start()
            return 0

        lax.fori_loop(0, chunks, relay, 0)

        def finish(i, _):
            own_copy(i).wait()
            near_copy(i).wait_send()
            near_arrival(i).wait_recv()
            for j in range(1, n_y):
                far_copy(j, i, y).wait_send()
                relay_copy(j, i, which).wait_send()
                relay_copy(j, i, 1 - which).wait_recv()
            return 0

        lax.fori_loop(0, chunks, finish, 0)
        for j, k in others:
            row_copy(j, k).wait_send()
            row_arrival(j, k).wait_recv()
        row_mine.wait()

    for which in range(CORES):
        pl.when(core == which)(functools.partial(path, which))


def exchange(number, keep, sel, buffer, hidden, n_grp, n_ep):
    n_y = n_grp // CORES
    most = max(keep)
    slots, columns = hidden.shape
    width = buffer.shape[2]
    chunks = pick_chunks(columns)
    rows = n_y * (keep[0] + keep[1])
    dma = pltpu.SemaphoreType.DMA
    return pl.pallas_call(
        functools.partial(exchange_kernel, n_grp, n_ep, keep),
        out_shape=(
            jax.ShapeDtypeStruct((rows, columns), hidden.dtype),
            jax.ShapeDtypeStruct((rows, width // n_grp), buffer.dtype),
        ),
        in_specs=[
            pl.BlockSpec(memory_space=pltpu.VMEM),
            pl.BlockSpec(memory_space=pl.ANY),
            pl.BlockSpec(memory_space=pltpu.VMEM),
        ],
        out_specs=(pl.BlockSpec(memory_space=pl.ANY), pl.BlockSpec(memory_space=pl.ANY)),
        scratch_shapes=[
            pltpu.VMEM((slots, width), buffer.dtype),
            pltpu.VMEM((most, columns), hidden.dtype),
            pltpu.VMEM((most, width), buffer.dtype),
            dma((n_ep,)), dma((n_ep,)), dma,
            dma((n_y, chunks)), dma((n_y, chunks)),
            dma((chunks,)), dma((chunks,)),
            dma((n_y, chunks)), dma((n_y, chunks)),
            dma((n_y, CORES)), dma((n_y, CORES)),
            dma((chunks + 1,)),
        ],
        compiler_params=pltpu.CompilerParams(
            collective_id=1 + number, has_side_effects=True, vmem_limit_bytes=60 * 1024 * 1024),
        name=f"exchange_{number}",
    )(sel, buffer, hidden)


def device_slots(d_rows, route_rows, weight_rows, alive):
    tokens_here, top = route_rows.shape
    scaled = weight_rows * alive[:, None]
    weighted = (d_rows.astype(jnp.float32)[:, None, :] * scaled[:, :, None]).astype(jnp.bfloat16)
    weighted = weighted.reshape(tokens_here * top, d_rows.shape[1])
    flat = route_rows.reshape(-1)
    chosen = (flat[:, None] == jnp.arange(EXPERTS, dtype=jnp.int32)[None, :]).astype(jnp.int32)
    before = jnp.cumsum(chosen, axis=0, dtype=jnp.int32) - chosen
    position = jnp.sum(before * chosen, axis=1, dtype=jnp.int32)
    slot_index = flat * CAP + position
    placing = (jnp.arange(EXPERTS * CAP, dtype=jnp.int32)[:, None] == slot_index[None, :]).astype(jnp.bfloat16)
    buffer = jnp.dot(placing, weighted, preferred_element_type=jnp.float32).astype(jnp.bfloat16)
    return buffer.reshape(EXPERTS, CAP, d_rows.shape[1])


def on_device(d_out, routes, combine, live_tokens, hidden):
    n_grp, n_ep = lax.axis_size("grp"), lax.axis_size("ep")
    shards = n_ep // EXPERTS
    grp, my_expert = lax.axis_index("grp"), lax.axis_index("ep") // shards
    slots = hidden.shape[0]
    alive = (jnp.arange(d_out.shape[0], dtype=jnp.int32) < live_tokens[0]).astype(jnp.float32)
    lanes = jnp.arange(128, dtype=jnp.int32)
    hits = (routes[:, :, None] == lanes[None, None, :]).astype(jnp.float32) * alive[:, None, None]
    counts = jnp.broadcast_to(jnp.sum(hits, axis=(0, 1))[None, :], (8, 128))
    table = share_counts(counts, n_grp, n_ep)[:, 0, :EXPERTS].reshape(n_grp, n_ep, EXPERTS)
    used = jnp.sum(table, axis=1)
    mine = (jnp.arange(EXPERTS, dtype=jnp.int32) == my_expert).astype(jnp.float32)
    scale = lax.rsqrt(1.0 + jnp.sum(used * mine[None, :]))
    here = (jnp.arange(n_grp, dtype=jnp.int32) == grp).astype(jnp.float32)
    filled = jnp.sum(table * mine * here[:, None, None], axis=(0, 2))
    first = jnp.cumsum(filled) - filled
    place = jnp.arange(CAP, dtype=jnp.float32)
    target = jnp.where(place[None, :] < filled[:, None], first[:, None] + place[None, :], -1.0).reshape(-1)
    sel = (jnp.arange(slots, dtype=jnp.float32)[:, None] == target[None, :]).astype(jnp.bfloat16)
    buffer = device_slots(d_out, routes, combine, alive)

    step = slots // 24
    sizes = ((17 * step, 21 * step), (24 * step, 24 * step))
    need = jnp.max(used.reshape(n_grp // CORES, CORES, EXPERTS), axis=(0, 2))
    fits = [jnp.all(need <= jnp.array(keep, jnp.float32)) for keep in sizes[:-1]]
    branch = len(sizes) - 1 - sum(f.astype(jnp.int32) for f in fits)

    def run(number, sel, buffer, hidden, scale):
        keep = sizes[number]
        all_hidden, all_rows = exchange(number, keep, sel[: max(keep)], buffer, hidden, n_grp, n_ep)
        total = lax.dot_general(all_rows, all_hidden, (((0,), (0,)), ((), ())), preferred_element_type=jnp.float32)
        return total * scale

    return lax.switch(branch, [functools.partial(run, n) for n in range(len(sizes))], sel, buffer, hidden, scale)


def solution(mesh):
    return jax.shard_map(
        on_device,
        mesh=mesh,
        in_specs=(
            P(("grp", "ep"), None),
            P(("grp", "ep"), None),
            P(("grp", "ep"), None),
            P(("grp", "ep")),
            P("grp", "ep"),
        ),
        out_specs=P("grp", "ep"),
        check_vma=False,
    )
```

```python
import functools

import jax
import jax.numpy as jnp
from jax import lax
from jax.experimental import pallas as pl
from jax.experimental.pallas import tpu as pltpu
from jax.sharding import PartitionSpec as P

EXPERTS = 8
CAP = 48
CORES = 2
CHUNKS = 7
MESH = pl.DeviceIdType.MESH


def pick_chunks(columns):
    return CHUNKS if columns % (CHUNKS * 128) == 0 else 1


def counts_kernel(n_grp, n_ep, ladder, router, live, sel, info, table, grp_send, grp_recv, ep_send, ep_recv):
    grp, ep = lax.axis_index("grp"), lax.axis_index("ep")
    shards = n_ep // EXPERTS
    barrier = pltpu.get_barrier_semaphore()

    def in_grp(j):
        return {"grp": lax.rem(grp + j, n_grp), "ep": ep}

    def in_ep(j):
        return {"grp": grp, "ep": lax.rem(ep + j, n_ep)}

    for j in range(1, n_grp):
        pl.semaphore_signal(barrier, inc=1, device_id=in_grp(j), device_id_type=MESH)
    for j in range(1, n_ep):
        pl.semaphore_signal(barrier, inc=1, device_id=in_ep(j), device_id_type=MESH)
    tokens, top = router.shape[0], router.shape[1] // 2
    lanes = lax.broadcasted_iota(jnp.int32, (tokens, 128), 1).astype(jnp.float32)
    alive = lax.broadcasted_iota(jnp.int32, (tokens, 128), 0) < live[0]
    hits = jnp.zeros((tokens, 128), jnp.float32)
    for k in range(top):
        hits = hits + jnp.where((router[:, k : k + 1] == lanes) & alive, 1.0, 0.0)
    table[ep, grp] = jnp.broadcast_to(jnp.sum(hits, axis=0, keepdims=True), (8, 128))
    pl.semaphore_wait(barrier, n_grp - 1 + n_ep - 1)

    def grp_copy(j, owner):
        part = table.at[ep, owner]
        return pltpu.make_async_remote_copy(
            src_ref=part, dst_ref=part, send_sem=grp_send.at[j], recv_sem=grp_recv.at[j],
            device_id=in_grp(j), device_id_type=MESH)

    def ep_copy(j, owner):
        part = table.at[owner]
        return pltpu.make_async_remote_copy(
            src_ref=part, dst_ref=part, send_sem=ep_send.at[j], recv_sem=ep_recv.at[j],
            device_id=in_ep(j), device_id_type=MESH)

    for j in range(1, n_grp):
        grp_copy(j, grp).start()
    for j in range(1, n_grp):
        grp_copy(j, lax.rem(grp - j + n_grp, n_grp)).wait_recv()
    for j in range(1, n_ep):
        ep_copy(j, ep).start()
    for j in range(1, n_ep):
        ep_copy(j, lax.rem(ep - j + n_ep, n_ep)).wait_recv()

    mine = lax.broadcasted_iota(jnp.int32, (1, 128), 1) == ep // shards
    slots = sel.shape[1]
    slot = lax.broadcasted_iota(jnp.int32, (1, slots), 1)
    source = slot // CAP
    place = (slot - source * CAP).astype(jnp.float32)
    filled = jnp.zeros((1, slots), jnp.float32)
    first = jnp.zeros((1, slots), jnp.float32)
    for s in range(n_ep):
        amount = jnp.sum(jnp.where(mine, table[s, grp, 0:1, :], 0.0), axis=1, keepdims=True)
        filled = filled + jnp.where(source == s, amount, 0.0)
        first = first + jnp.where(source > s, amount, 0.0)
    target = jnp.where(place < filled, first + place, -1.0)
    rows = 64 if slots % 64 == 0 else slots

    def write(i, _):
        start = pl.multiple_of(i * rows, rows)
        index = (lax.broadcasted_iota(jnp.int32, (rows, slots), 0) + start).astype(jnp.float32)
        sel[pl.ds(start, rows), :] = jnp.where(index == target, 1.0, 0.0).astype(sel.dtype)
        return 0

    lax.fori_loop(0, slots // rows, write, 0)
    need = [jnp.zeros((1, 128), jnp.float32) for _ in range(CORES)]
    count = jnp.zeros((1, 128), jnp.float32)
    for g in range(n_grp):
        used = jnp.zeros((1, 128), jnp.float32)
        for s in range(n_ep):
            used = used + table[s, g, 0:1, :]
        need[g % CORES] = jnp.maximum(need[g % CORES], used)
        count = count + used
    count = jnp.sum(jnp.where(mine, count, 0.0), axis=1, keepdims=True)
    need = [jnp.max(n, axis=1, keepdims=True) for n in need]
    branch = jnp.zeros((1, 1), jnp.float32)
    for keep in ladder:
        branch = branch + jnp.where((need[0] <= keep[0]) & (need[1] <= keep[1]), 0.0, 1.0)
    lane = lax.broadcasted_iota(jnp.int32, (8, 128), 1)
    info[...] = jnp.where(lane == 0, branch, count)
    for j in range(1, n_grp):
        grp_copy(j, grp).wait_send()
    for j in range(1, n_ep):
        ep_copy(j, ep).wait_send()


def share_counts(router, live, slots, ladder, n_grp, n_ep):
    dma = pltpu.SemaphoreType.DMA
    return pl.pallas_call(
        functools.partial(counts_kernel, n_grp, n_ep, ladder),
        out_shape=(
            jax.ShapeDtypeStruct((slots, slots), jnp.bfloat16),
            jax.ShapeDtypeStruct((8, 128), jnp.float32),
        ),
        in_specs=[pl.BlockSpec(memory_space=pltpu.VMEM), pl.BlockSpec(memory_space=pltpu.SMEM)],
        out_specs=(pl.BlockSpec(memory_space=pltpu.VMEM), pl.BlockSpec(memory_space=pltpu.VMEM)),
        scratch_shapes=[
            pltpu.VMEM((n_ep, n_grp, 8, 128), jnp.float32),
            dma((n_grp,)), dma((n_grp,)), dma((n_ep,)), dma((n_ep,)),
        ],
        compiler_params=pltpu.CompilerParams(collective_id=0, has_side_effects=True),
        name="share_counts",
    )(router, live)


def exchange_kernel(n_grp, n_ep, keep, sel, d_out, router, live, hidden, all_hidden, all_rows, buffer, arrived, packed, packed_rows,
                    slot_send, slot_recv, slot_own, far_send, far_recv, near_send, near_recv,
                    relay_send, relay_recv, row_send, row_recv, own_sem):
    n_y = n_grp // CORES
    grp, ep = lax.axis_index("grp"), lax.axis_index("ep")
    shards = n_ep // EXPERTS
    y = grp // CORES
    core = lax.rem(grp, CORES)
    pair = keep[0] + keep[1]
    chunks = pick_chunks(hidden.shape[1])
    wide = hidden.shape[1] // chunks
    block = all_rows.shape[1]

    barrier = pltpu.get_barrier_semaphore()

    def greet_ep(j, _):
        pl.semaphore_signal(barrier, inc=1, device_id={"grp": grp, "ep": lax.rem(ep + j, n_ep)}, device_id_type=MESH)
        return 0

    def greet_grp(j, _):
        pl.semaphore_signal(barrier, inc=1, device_id={"grp": lax.rem(grp + j, n_grp), "ep": ep}, device_id_type=MESH)
        return 0

    lax.fori_loop(1, n_ep, greet_ep, 0)
    lax.fori_loop(1, n_grp, greet_grp, 0)
    pl.semaphore_wait(barrier, n_ep - 1 + n_grp - 1)

    def expert_slots(expert):
        return buffer.at[pl.ds(pl.multiple_of(expert * CAP, CAP), CAP), :]

    def slot_copy(j, source):
        target = lax.rem(ep + j, n_ep)
        return pltpu.make_async_remote_copy(
            src_ref=expert_slots(target // shards),
            dst_ref=arrived.at[pl.ds(pl.multiple_of(source * CAP, CAP), CAP), :],
            send_sem=slot_send.at[j], recv_sem=slot_recv.at[j],
            device_id={"grp": grp, "ep": target}, device_id_type=MESH)

    def slot_start(j, _):
        slot_copy(j, ep).start()
        return 0

    def slot_finish(j, _):
        slot_copy(j, ep).wait_send()
        slot_copy(j, lax.rem(ep - j + n_ep, n_ep)).wait_recv()
        return 0

    slot_mine = pltpu.make_async_copy(
        expert_slots(ep // shards), arrived.at[pl.ds(pl.multiple_of(ep * CAP, CAP), CAP), :], slot_own)

    def fill_slots():
        tokens, top = router.shape[0], router.shape[1] // 2
        lanes = lax.broadcasted_iota(jnp.int32, (tokens, 128), 1).astype(jnp.float32)
        alive = jnp.where(lax.broadcasted_iota(jnp.int32, (tokens, 1), 0) < live[0], 1.0, 0.0)
        chosen = [jnp.where(router[:, k : k + 1] == lanes, 1.0, 0.0) for k in range(top)]
        square = (tokens, tokens)
        earlier = jnp.where(
            lax.broadcasted_iota(jnp.int32, square, 0) > lax.broadcasted_iota(jnp.int32, square, 1), 1.0, 0.0)
        running = jnp.dot(
            earlier.astype(jnp.bfloat16), sum(chosen).astype(jnp.bfloat16), preferred_element_type=jnp.float32)
        slot = lax.broadcasted_iota(jnp.int32, (tokens, EXPERTS * CAP), 1).astype(jnp.float32)
        puts, weights = [], []
        for k in range(top):
            position = jnp.sum(chosen[k] * running, axis=1, keepdims=True)
            running = running + chosen[k]
            place = router[:, k : k + 1] * CAP + position
            puts.append(jnp.where(slot == place, 1.0, 0.0).astype(jnp.bfloat16))
            weights.append(router[:, top + k : top + k + 1] * alive)
        for i in range(n_grp):
            part = slice(i * block, (i + 1) * block)
            rows = d_out[:, part].astype(jnp.float32)
            buffer[:, part] = sum(
                lax.dot_general(
                    put, (rows * weight).astype(jnp.bfloat16), (((0,), (0,)), ((), ())),
                    preferred_element_type=jnp.float32)
                for put, weight in zip(puts, weights)).astype(d_out.dtype)

    def path(which):
        mine, other = keep[which], keep[1 - which]
        mate = y * CORES + (1 - which)

        def span(row, cell):
            start = row * pair + (0 if cell == 0 else keep[0])
            return pl.ds(pl.multiple_of(start, 16), keep[cell])

        def columns(i):
            return pl.ds(pl.multiple_of(i * wide, 128), wide)

        def at_y(j):
            return {"grp": lax.rem(y + j, n_y) * CORES + which, "ep": ep}

        def own_copy(i):
            return pltpu.make_async_copy(
                packed.at[pl.ds(0, mine), columns(i)], all_hidden.at[span(y, which), columns(i)], own_sem.at[i])

        def far_copy(j, i, row):
            return pltpu.make_async_remote_copy(
                src_ref=packed.at[pl.ds(0, mine), columns(i)], dst_ref=all_hidden.at[span(row, which), columns(i)],
                send_sem=far_send.at[j, i], recv_sem=far_recv.at[j, i], device_id=at_y(j), device_id_type=MESH)

        def near_copy(i):
            return pltpu.make_async_remote_copy(
                src_ref=packed.at[pl.ds(0, mine), columns(i)], dst_ref=all_hidden.at[span(y, which), columns(i)],
                send_sem=near_send.at[i], recv_sem=near_recv.at[i],
                device_id={"grp": mate, "ep": ep}, device_id_type=MESH)

        def near_arrival(i):
            return pltpu.make_async_remote_copy(
                src_ref=all_hidden.at[span(y, 1 - which), columns(i)],
                dst_ref=all_hidden.at[span(y, 1 - which), columns(i)],
                send_sem=near_send.at[i], recv_sem=near_recv.at[i],
                device_id={"grp": mate, "ep": ep}, device_id_type=MESH)

        def relay_copy(j, i, cell):
            row = lax.rem(y - j + n_y, n_y)
            return pltpu.make_async_remote_copy(
                src_ref=all_hidden.at[span(row, cell), columns(i)], dst_ref=all_hidden.at[span(row, cell), columns(i)],
                send_sem=relay_send.at[j, i], recv_sem=relay_recv.at[j, i],
                device_id={"grp": mate, "ep": ep}, device_id_type=MESH)

        def row_copy(j, k):
            cell = which if k == 0 else 1 - which
            target = lax.rem(y + j, n_y) * CORES + cell
            return pltpu.make_async_remote_copy(
                src_ref=packed_rows.at[pl.ds(0, mine), pl.ds(pl.multiple_of(target * block, 128), block)],
                dst_ref=all_rows.at[span(y, which), :],
                send_sem=row_send.at[j, k], recv_sem=row_recv.at[j, k],
                device_id={"grp": target, "ep": ep}, device_id_type=MESH)

        def row_arrival(j, k):
            cell = which if k == 0 else 1 - which
            here = all_rows.at[span(lax.rem(y - j + n_y, n_y), cell), :]
            return pltpu.make_async_remote_copy(
                src_ref=here, dst_ref=here, send_sem=row_send.at[j, k], recv_sem=row_recv.at[j, k],
                device_id={"grp": lax.rem(grp + 1, n_grp), "ep": ep}, device_id_type=MESH)

        others = [(j, k) for j in range(n_y) for k in range(CORES) if (j, k) != (0, 0)]

        def start(i):
            for j in range(1, n_y):
                far_copy(j, i, y).start()
            near_copy(i).start()
            own_copy(i).start()

        def pack(i, _):
            packed[pl.ds(0, mine), columns(i)] = jnp.dot(
                sel[pl.ds(0, mine), :], hidden[:, columns(i)], preferred_element_type=jnp.float32).astype(packed.dtype)

            @pl.when(i > 0)
            def _():
                start(i - 1)

            return 0

        def relay(i, _):
            for j in range(1, n_y):
                far_copy(j, i, lax.rem(y - j + n_y, n_y)).wait_recv()
                relay_copy(j, i, which).start()
            return 0

        stops = [min(i, chunks) for i in range(4)] + [chunks]
        lax.fori_loop(0, chunks, pack, 0)
        fill_slots()
        start(chunks - 1)
        lax.fori_loop(stops[0], stops[1], relay, 0)
        lax.fori_loop(1, n_ep, slot_start, 0)
        slot_mine.start()
        lax.fori_loop(stops[1], stops[2], relay, 0)
        lax.fori_loop(1, n_ep, slot_finish, 0)
        slot_mine.wait()

        def pack_rows(i, _):
            part = pl.ds(pl.multiple_of(i * block, 128), block)
            packed_rows[pl.ds(0, mine), part] = jnp.dot(
                sel[pl.ds(0, mine), :], arrived[:, part], preferred_element_type=jnp.float32).astype(packed_rows.dtype)
            return 0

        lax.fori_loop(0, n_grp, pack_rows, 0)
        lax.fori_loop(stops[2], stops[3], relay, 0)
        row_mine = pltpu.make_async_copy(
            packed_rows.at[pl.ds(0, mine), pl.ds(pl.multiple_of(grp * block, 128), block)],
            all_rows.at[span(y, which), :], own_sem.at[chunks])
        for j, k in others:
            row_copy(j, k).start()
        row_mine.start()

        lax.fori_loop(stops[3], stops[4], relay, 0)

        def finish(i, _):
            own_copy(i).wait()
            near_copy(i).wait_send()
            near_arrival(i).wait_recv()
            for j in range(1, n_y):
                far_copy(j, i, y).wait_send()
                relay_copy(j, i, which).wait_send()
                relay_copy(j, i, 1 - which).wait_recv()
            return 0

        lax.fori_loop(0, chunks, finish, 0)
        for j, k in others:
            row_copy(j, k).wait_send()
            row_arrival(j, k).wait_recv()
        row_mine.wait()

    for which in range(CORES):
        pl.when(core == which)(functools.partial(path, which))


def exchange(number, keep, sel, d_out, router, live, hidden, n_grp, n_ep):
    n_y = n_grp // CORES
    most = max(keep)
    slots, columns = hidden.shape
    width = d_out.shape[1]
    chunks = pick_chunks(columns)
    rows = n_y * (keep[0] + keep[1])
    dma = pltpu.SemaphoreType.DMA
    return pl.pallas_call(
        functools.partial(exchange_kernel, n_grp, n_ep, keep),
        out_shape=(
            jax.ShapeDtypeStruct((rows, columns), hidden.dtype),
            jax.ShapeDtypeStruct((rows, width // n_grp), d_out.dtype),
        ),
        in_specs=[
            pl.BlockSpec(memory_space=pltpu.VMEM),
            pl.BlockSpec(memory_space=pltpu.VMEM),
            pl.BlockSpec(memory_space=pltpu.VMEM),
            pl.BlockSpec(memory_space=pltpu.SMEM),
            pl.BlockSpec(memory_space=pltpu.VMEM),
        ],
        out_specs=(pl.BlockSpec(memory_space=pl.ANY), pl.BlockSpec(memory_space=pl.ANY)),
        scratch_shapes=[
            pltpu.VMEM((EXPERTS * CAP, width), d_out.dtype),
            pltpu.VMEM((slots, width), d_out.dtype),
            pltpu.VMEM((most, columns), hidden.dtype),
            pltpu.VMEM((most, width), d_out.dtype),
            dma((n_ep,)), dma((n_ep,)), dma,
            dma((n_y, chunks)), dma((n_y, chunks)),
            dma((chunks,)), dma((chunks,)),
            dma((n_y, chunks)), dma((n_y, chunks)),
            dma((n_y, CORES)), dma((n_y, CORES)),
            dma((chunks + 1,)),
        ],
        compiler_params=pltpu.CompilerParams(
            collective_id=1 + number, has_side_effects=True, vmem_limit_bytes=60 * 1024 * 1024),
        name=f"exchange_{number}",
    )(sel, d_out, router, live, hidden)


def on_device(d_out, routes, combine, live_tokens, hidden):
    n_grp, n_ep = lax.axis_size("grp"), lax.axis_size("ep")
    slots = hidden.shape[0]
    step = slots // 24
    sizes = ((17 * step, 21 * step), (24 * step, 24 * step))
    router = jnp.concatenate([routes.astype(jnp.float32), combine], axis=1)
    sel, info = share_counts(router, live_tokens, slots, sizes[:-1], n_grp, n_ep)
    branch = info[0, 0].astype(jnp.int32)
    count = info[0, 1]

    def run(number, *operands):
        *sources, count = operands
        all_hidden, all_rows = exchange(number, sizes[number], *sources, n_grp, n_ep)
        total = lax.dot_general(all_rows, all_hidden, (((0,), (0,)), ((), ())), preferred_element_type=jnp.float32)
        return total * lax.rsqrt(1.0 + count)

    branches = [functools.partial(run, n) for n in range(len(sizes))]
    return lax.switch(branch, branches, sel, d_out, router, live_tokens, hidden, count)


def solution(mesh):
    return jax.shard_map(
        on_device,
        mesh=mesh,
        in_specs=(
            P(("grp", "ep"), None),
            P(("grp", "ep"), None),
            P(("grp", "ep"), None),
            P(("grp", "ep")),
            P("grp", "ep"),
        ),
        out_specs=P("grp", "ep"),
        check_vma=False,
    )
```
